32 devices in a mesh: blk: 8 (over z, core), grp: 4 (over y, x).
Axes of the slice: x: 2, y: 2, z: 4, core: 2. Of those that a mesh axis runs over, the one named last changes fastest.
Arguments:
- images: bfloat16 [4, 2048, 1152], P('grp', 'blk'), may hold values from -1 to 1
- texts: bfloat16 [4, 2048, 1152], P('grp', 'blk'), may hold values from -1 to 1
- labels: int32 [4, 8, 256], P('grp', 'blk'), may hold values from 0 to 255, each once within a row
- partners: int32 [2, 8], replicated, may hold values from 0 to 7, as said below
- logit_scale: float32 [], replicated, may hold values from 1 to 3
- logit_bias: float32 [], replicated, may hold values from -3 to -1
Outputs:
- image_grad: float32 [4, 2048, 1152], P('grp', 'blk')
- text_grad: float32 [4, 2048, 1152], P('grp', 'blk')
- loss: float32 [], replicated
The draws below stay inside these ranges and needn't reach their ends.
Inputs may be any that keep to these rules, and one draw needn't show every extreme that they name: Each block's labels are a permutation of its 256 text rows. partners[r, i] is block i's partner in round r: partners[r, partners[r, i]] == i and partners[r, i] != i; no two rounds pair the same two blocks.
All inputs are finite; a program needn't handle non-finite values.
Results may differ from the reference program's by a relative error of at most 0.00035.
The reference program's roundings to bfloat16 on the way (of `weight`) count: a program that leaves them out, or rounds other values in their place, can miss the bound.
Values may be sent and summed in bfloat16 or wider, within the bound.
A program may use at most 64 MiB of HBM per device.

```python
import math
import jax
import jax.numpy as jnp
from jax import lax

D = 1152
ROWS = 256
ROUNDS = 2
BLOCKS = 8
GROUPS = 4
BATCH_G = 2048


def draw_partners(key, part):
    cycle = BLOCKS - 1
    order = jax.random.permutation(jax.random.fold_in(key, 11), BLOCKS).astype(jnp.int32)
    picks = jax.random.permutation(jax.random.fold_in(key, 12), cycle)[:ROUNDS].astype(jnp.int32)
    slots = jnp.arange(BLOCKS, dtype=jnp.int32)

    def one_round(pick):
        other = jnp.where(slots == pick, cycle, (2 * pick - slots) % cycle)
        other = jnp.where(slots == cycle, pick, other).astype(jnp.int32)
        return jnp.zeros((BLOCKS,), jnp.int32).at[order].set(order[other])
    return jax.vmap(one_round)(picks).astype(jnp.int32)


def level_of(key, shape, pieces, least, top_value):
    gain, own = 1.0, jax.random.fold_in(key, 6)
    for position, parts in pieces:
        steps = jnp.exp(jax.random.uniform(jax.random.fold_in(own, position), (parts,), jnp.float32, least / len(pieces), top_value / len(pieces)))
        gain = gain * jnp.repeat(steps, shape[position] // parts).reshape([-1 if axis == position else 1 for axis in range(len(shape))])
    return gain


def gaussian(rng, dims, spread, bound, cuts=(), kind=jnp.bfloat16):
    result = jax.random.normal(rng, dims, jnp.float32) * spread
    if len(cuts) > 0:
        result = level_of(rng, dims, cuts, -0.22, 0.18) * result
    return jnp.clip(result, min=-bound, max=bound).astype(kind)


def setup_inputs(seed: int = 0) -> dict:
    seeds = jax.random.split(jax.random.key(seed), 7)
    images = gaussian(seeds[0], (GROUPS, BATCH_G, D), 0.17, 1.0, ((0, 4), (1, 8)))
    texts = gaussian(seeds[1], (GROUPS, BATCH_G, D), 0.17, 1.0, ((0, 4), (1, 8)))
    labels = jax.vmap(lambda own: jax.random.permutation(own, ROWS))(jax.random.split(seeds[2], GROUPS * BLOCKS)).reshape((GROUPS, BLOCKS, ROWS)).astype(jnp.int32)
    partners = draw_partners(jax.random.fold_in(seeds[6], 71), 0)
    logit_scale = jnp.clip(jnp.exp(jax.random.uniform(seeds[4], (), jnp.float32, math.log(1.0), math.log(3.0))), 1.0, 3.0)
    logit_bias = jnp.clip(jax.random.uniform(seeds[5], (), jnp.float32, -3.0, -1.0), -3.0, -1.0)
    return {"images": images, "texts": texts, "labels": labels, "partners": partners, "logit_scale": logit_scale, "logit_bias": logit_bias}


def pair_terms(image_rows, text_rows, positive, logit_scale, logit_bias):
    logits = logit_scale * jnp.dot(image_rows, text_rows.T, preferred_element_type=jnp.float32) + logit_bias
    signed = jnp.where(positive, jnp.float32(1.0), jnp.float32(-1.0))
    loss_sum = jnp.sum(jax.nn.softplus(-signed * logits))
    weight = (-signed * jax.nn.sigmoid(-signed * logits)).astype(jnp.bfloat16)
    image_part = logit_scale * jnp.dot(weight, text_rows, preferred_element_type=jnp.float32)
    text_part = logit_scale * jnp.dot(weight.T, image_rows, preferred_element_type=jnp.float32)
    return loss_sum, image_part, text_part


def reference(images, texts, labels, partners, logit_scale, logit_bias):
    columns = jnp.arange(ROWS, dtype=jnp.int32)
    nothing = jnp.zeros((ROWS, ROWS), dtype=bool)

    def one_group(operands):
        group_images, group_texts, group_labels = operands
        image_blocks = group_images.reshape(BLOCKS, ROWS, D)
        text_blocks = group_texts.reshape(BLOCKS, ROWS, D)
        positive = group_labels[:, :, None] == columns[None, None, :]
        losses, image_acc, text_acc = lax.map(
            lambda item: pair_terms(item[0], item[1], item[2], logit_scale, logit_bias),
            (image_blocks, text_blocks, positive))
        loss_sum = jnp.sum(losses)
        for round_index in range(ROUNDS):
            partner_row = partners[round_index].astype(jnp.int32)
            cross_loss, cross_image, cross_text = lax.map(
                lambda item: pair_terms(item[0], item[1], nothing, logit_scale, logit_bias),
                (image_blocks, text_blocks[partner_row]))
            loss_sum = loss_sum + jnp.sum(cross_loss)
            image_acc = image_acc + cross_image
            text_acc = text_acc + cross_text[partner_row]
        return loss_sum, image_acc.reshape(BATCH_G, D), text_acc.reshape(BATCH_G, D)

    group_losses, image_grad, text_grad = lax.map(one_group, (images, texts, labels))
    loss = jnp.sum(group_losses) / jnp.float32(GROUPS * BATCH_G)
    return image_grad, text_grad, loss
```

```python
import functools
import jax
import jax.numpy as jnp
from jax import lax
from jax.experimental import pallas as pl
from jax.experimental.pallas import tpu as pltpu
from jax.sharding import PartitionSpec as P

MESH = pl.DeviceIdType.MESH
CHUNK_ROWS = 32
VMEM_BUDGET = 48 * 1024 * 1024
VMEM_LIMIT = 60 * 1024 * 1024


def block_weights(image_rows, text_rows, positive, logit_scale, logit_bias):
    logits = (
        logit_scale * jnp.dot(image_rows, text_rows.T, preferred_element_type=jnp.float32)
        + logit_bias
    )
    signed = jnp.where(positive, jnp.float32(1.0), jnp.float32(-1.0))
    loss_sum = jnp.sum(jax.nn.softplus(-signed * logits))
    weight = (-signed * jax.nn.sigmoid(-signed * logits)).astype(jnp.bfloat16)
    return (loss_sum, weight)


def regroup(received, partner_row):
    row_count, width = received.shape
    devices = partner_row.shape[0]
    pieces = received.reshape(row_count, devices, width // devices)
    pieces = jnp.take(pieces, partner_row, axis=1)
    return pieces.reshape(row_count, width)


def spread_body(images, texts, labels, partners, logit_scale, logit_bias):
    own_images = images[0]
    own_texts = texts[0]
    row_count = own_images.shape[0]
    columns = jnp.arange(row_count, dtype=jnp.int32)
    positive = labels[0, 0][:, None] == columns[None, :]
    nothing = jnp.zeros((row_count, row_count), dtype=bool)
    loss_sum, weight = block_weights(own_images, own_texts, positive, logit_scale, logit_bias)
    image_grad = logit_scale * jnp.dot(weight, own_texts, preferred_element_type=jnp.float32)
    text_grad = logit_scale * jnp.dot(weight.T, own_images, preferred_element_type=jnp.float32)
    for round_index in range(partners.shape[0]):
        partner_row = partners[round_index]
        spread_images, spread_texts = (
            lax.all_to_all(own_images, "blk", split_axis=1, concat_axis=1, tiled=True),
            lax.all_to_all(own_texts, "blk", split_axis=1, concat_axis=1, tiled=True),
        )
        their_images, their_texts = (
            lax.all_to_all(
                regroup(spread_images, partner_row), "blk", split_axis=1, concat_axis=1, tiled=True
            ),
            lax.all_to_all(
                regroup(spread_texts, partner_row), "blk", split_axis=1, concat_axis=1, tiled=True
            ),
        )
        round_loss, weight = block_weights(
            own_images, their_texts, nothing, logit_scale, logit_bias
        )
        image_grad = image_grad + logit_scale * jnp.dot(
            weight, their_texts, preferred_element_type=jnp.float32
        )
        _, mirror = block_weights(
            their_images, own_texts, nothing, logit_scale, logit_bias
        )
        text_grad = text_grad + logit_scale * jnp.dot(
            mirror.T, their_images, preferred_element_type=jnp.float32
        )
        loss_sum = loss_sum + round_loss
    loss_all = lax.psum(loss_sum, ("blk", "grp"))
    image_count = lax.axis_size("blk") * lax.axis_size("grp") * row_count
    loss = loss_all / jnp.float32(image_count)
    return (image_grad[None], text_grad[None], loss)


def logistic_terms(value):
    small = jnp.exp(-jnp.abs(value))
    inverse = 1.0 / (1.0 + small)
    weight = jnp.where(value >= 0, inverse, small * inverse)
    return weight, jnp.maximum(value, 0.0) + jnp.log1p(small)


def rows_dot(rows, own):
    return lax.dot_general(rows, own, (((1,), (1,)), ((), ())), preferred_element_type=jnp.float32)


def weight_dot(weight, rows):
    return lax.dot_general(
        weight, rows, (((0,), (0,)), ((), ())), preferred_element_type=jnp.float32
    )


def fold(terms):
    rows, columns = terms.shape
    total = jnp.sum(terms.reshape(rows // 8, 8, columns), axis=0)
    return sum(total[:, c : c + 128] for c in range(0, columns, 128))


def exchange_kernel(
    n, groups, rounds, edges,
    partners_ref, scale_ref, bias_ref, labels_ref, images_ref, texts_ref,
    image_acc, text_acc, loss_ref,
    own, loss_sum, group_loss, block_loss,
    own_sem, load_sem, recv_sem, send_sem, slot_sem,
    group_send, group_recv, block_send, block_recv, *buffers,
):
    chunks = len(edges) - 1
    held, slots = buffers[:chunks], buffers[chunks:]
    chips = n // 2
    me = lax.axis_index("blk")
    grp = lax.axis_index("grp")
    chip = lax.div(me, 2)
    core = lax.rem(me, 2)
    sibling = me + 1 - 2 * core
    inner = jnp.logical_and(chip > 0, chip < chips - 1)
    outer = jnp.logical_not(inner)
    up_all = chip < chips - 2
    down_all = chip > 1
    beside_end = jnp.logical_or(chip == 1, chip == chips - 2)
    end_device = jnp.where(chip == 1, me - 2, me + 2)
    scale = scale_ref[0]
    bias = bias_ref[0]

    loads = []
    for k in range(chunks):
        part = pl.ds(edges[k], edges[k + 1] - edges[k])
        loads.append([
            pltpu.make_async_copy(ref.at[0, part], held[k].at[me, i], load_sem.at[k, i])
            for i, ref in enumerate((images_ref, texts_ref))
        ])
        for copy in loads[-1]:
            copy.start()
    own_loads = [
        pltpu.make_async_copy(ref.at[0], own.at[i], own_sem.at[i])
        for i, ref in enumerate((images_ref, texts_ref))
    ]
    for copy in own_loads:
        copy.start()

    barrier = pltpu.get_barrier_semaphore()
    for step in range(1, n):
        pl.semaphore_signal(
            barrier, inc=1, device_id={"blk": lax.rem(me + step, n)}, device_id_type=MESH
        )
    for step in range(1, groups):
        pl.semaphore_signal(
            barrier, inc=1, device_id={"grp": lax.rem(grp + step, groups)}, device_id_type=MESH
        )
    pl.semaphore_wait(barrier, n - 1 + groups - 1)

    pending = []

    def copy_of(k, entry, way, target):
        return pltpu.make_async_remote_copy(
            src_ref=held[k].at[entry],
            dst_ref=held[k].at[entry],
            send_sem=send_sem.at[k, way, lax.div(entry, 2)],
            recv_sem=recv_sem.at[k, entry],
            device_id={"blk": target},
            device_id_type=MESH,
        )

    def send(k, entry, way, target, when):
        pending.append((when, lambda: copy_of(k, entry, way, target).wait_send()))
        pl.when(when)(lambda: copy_of(k, entry, way, target).start())

    def arrived(k, entry, when):
        pl.when(when)(lambda: copy_of(k, entry, 0, sibling).wait_recv())

    def send_own(k, when):
        send(k, me, 0, me + 2, jnp.logical_and(when, up_all))
        send(k, me, 1, me - 2, jnp.logical_and(when, down_all))
        send(k, me, 2, sibling, jnp.logical_and(when, inner))

    def relay(k, passing):
        for distance in range(1, chips - 1):
            below = jnp.logical_and(inner, chip >= distance)
            below = jnp.logical_and(below, up_all == passing)
            arrived(k, me - 2 * distance, below)
            if passing:
                send(k, me - 2 * distance, 0, me + 2, below)
            send(k, me - 2 * distance, 2, sibling, below)
            above = jnp.logical_and(inner, chip + distance < chips)
            above = jnp.logical_and(above, down_all == passing)
            arrived(k, me + 2 * distance, above)
            if passing:
                send(k, me + 2 * distance, 1, me - 2, above)
            send(k, me + 2 * distance, 2, sibling, above)

    def slot_copy(k):
        return pltpu.make_async_remote_copy(
            src_ref=slots[k],
            dst_ref=held[k].at[pl.ds(n, rounds)],
            send_sem=slot_sem.at[k],
            recv_sem=recv_sem.at[k, n],
            device_id={"blk": end_device},
            device_id_type=MESH,
        )

    def select(k):
        for at in range(chips):
            arrived(k, 2 * at + 1 - core, inner)

        @pl.when(beside_end)
        def _():
            for r in range(rounds):
                slots[k][r] = held[k][partners_ref[r, end_device]]
            slot_copy(k).start()

        pl.when(outer)(lambda: slot_copy(k).wait_recv())

    def compute(k):
        found = [
            held[k][jnp.where(inner, partners_ref[r, me], n + r)] for r in range(rounds)
        ]
        their_images = jnp.concatenate([rows[0] for rows in found], axis=0)
        their_texts = jnp.concatenate([rows[1] for rows in found], axis=0)
        weight, terms = logistic_terms(scale * rows_dot(their_texts, own[0]) + bias)
        loss_sum[...] += fold(terms)
        mirror, _ = logistic_terms(scale * rows_dot(their_images, own[1]) + bias)
        image_acc[0] += weight_dot(weight.astype(jnp.bfloat16), their_texts)
        text_acc[0] += weight_dot(mirror.astype(jnp.bfloat16), their_images)

    always = me >= 0
    for k in range(chunks):
        for copy in loads[k]:
            copy.wait()
        send_own(k, always if k < 2 else outer)

    for copy in own_loads:
        copy.wait()
    logits = scale * rows_dot(own[1], own[0]) + bias
    positive = lax.broadcasted_iota(jnp.int32, logits.shape, 0) == labels_ref[0]
    signed = jnp.where(positive, -1.0, 1.0)
    weight, terms = logistic_terms(signed * logits)
    weight = (signed * weight).astype(jnp.bfloat16)
    loss_sum[...] = fold(terms)
    image_acc[0] = weight_dot(weight, own[1])
    text_acc[0] = jnp.dot(weight, own[0], preferred_element_type=jnp.float32)

    relay(0, True)
    for k in range(chunks):
        if k + 1 < chunks:
            relay(k + 1, True)
        if k + 2 < chunks:
            send_own(k + 2, inner)
        relay(k, False)
        select(k)
        compute(k)

    def share(slot, position, count, axis, send, recv):
        def copy(step):
            return pltpu.make_async_remote_copy(
                src_ref=slot.at[position],
                dst_ref=slot.at[position],
                send_sem=send.at[step],
                recv_sem=recv.at[position],
                device_id={axis: lax.rem(position + step, count)},
                device_id_type=MESH,
            )

        for step in range(1, count):
            copy(step).start()
        for step in range(1, count):
            other = lax.rem(position + step, count)
            pltpu.make_async_remote_copy(
                src_ref=slot.at[other],
                dst_ref=slot.at[other],
                send_sem=send.at[step],
                recv_sem=recv.at[other],
                device_id={axis: other},
                device_id_type=MESH,
            ).wait_recv()
        for step in range(1, count):
            copy(step).wait_send()
        total = slot[0]
        for at in range(1, count):
            total = total + slot[at]
        return total

    group_loss[grp] = loss_sum[...]
    block_loss[me] = share(group_loss, grp, groups, "grp", group_send, group_recv)
    total = share(block_loss, me, n, "blk", block_send, block_recv)
    loss_ref[0, 0] = jnp.sum(total) / jnp.float32(n * groups * own.shape[1])

    for when, wait in pending:
        pl.when(when)(wait)
    for k in range(chunks):
        pl.when(beside_end)(lambda k=k: slot_copy(k).wait_send())


def chunk_edges(rows):
    return list(range(0, rows, CHUNK_ROWS)) + [rows]


def gather_body(n, groups, images, texts, labels, partners, logit_scale, logit_bias):
    _, rows, width = images.shape
    rounds = partners.shape[0]
    edges = chunk_edges(rows)
    chunks = len(edges) - 1
    sizes = [edges[k + 1] - edges[k] for k in range(chunks)]
    vmem = pl.BlockSpec(memory_space=pltpu.VMEM)
    smem = pl.BlockSpec(memory_space=pltpu.SMEM)
    hbm = pl.BlockSpec(memory_space=pl.ANY)
    dma = pltpu.SemaphoreType.DMA
    grad = jax.ShapeDtypeStruct(images.shape, jnp.float32)
    image_grad, text_grad, loss = pl.pallas_call(
        functools.partial(exchange_kernel, n, groups, rounds, edges),
        out_shape=(grad, grad, jax.ShapeDtypeStruct((1, 1), jnp.float32)),
        in_specs=[smem, smem, smem, vmem, hbm, hbm],
        out_specs=(vmem, vmem, smem),
        scratch_shapes=[
            pltpu.VMEM((2, rows, width), images.dtype),
            pltpu.VMEM((8, 128), jnp.float32),
            pltpu.VMEM((groups, 8, 128), jnp.float32),
            pltpu.VMEM((n, 8, 128), jnp.float32),
            dma((2,)),
            dma((chunks, 2)),
            dma((chunks, n + 1)),
            dma((chunks, 3, n // 2)),
            dma((chunks,)),
            dma((groups,)),
            dma((groups,)),
            dma((n,)),
            dma((n,)),
        ]
        + [pltpu.VMEM((n + rounds, 2, size, width), images.dtype) for size in sizes]
        + [pltpu.VMEM((rounds, 2, size, width), images.dtype) for size in sizes],
        compiler_params=pltpu.CompilerParams(
            collective_id=0, has_side_effects=True, vmem_limit_bytes=VMEM_LIMIT
        ),
    )(partners, logit_scale.reshape(1), logit_bias.reshape(1), labels, images, texts)
    return logit_scale * image_grad, logit_scale * text_grad, loss.reshape(())


def solution(mesh):
    in_specs = (P("grp", "blk", None), P("grp", "blk", None), P("grp", "blk", None), P(), P(), P())
    out_specs = (P("grp", "blk", None), P("grp", "blk", None), P())
    n, groups = mesh.shape["blk"], mesh.shape["grp"]

    def body(images, texts, labels, partners, logit_scale, logit_bias):
        _, rows, width = images.shape
        rounds = partners.shape[0]
        block = 2 * rows * width * images.dtype.itemsize
        needed = block * (n + 2 * rounds + 1) + 2 * rows * width * 4
        fits = needed <= VMEM_BUDGET and n % 2 == 0 and n >= 8
        if fits and rows % CHUNK_ROWS == 0 and rows % 128 == 0 and width % 128 == 0:
            return gather_body(
                n, groups, images, texts, labels, partners, logit_scale, logit_bias
            )
        return spread_body(images, texts, labels, partners, logit_scale, logit_bias)

    return jax.shard_map(body, mesh=mesh, in_specs=in_specs, out_specs=out_specs, check_vma=False)
```

```python
import functools
import jax
import jax.numpy as jnp
from jax import lax
from jax.experimental import pallas as pl
from jax.experimental.pallas import tpu as pltpu
from jax.sharding import PartitionSpec as P

MESH = pl.DeviceIdType.MESH
CHUNK_ROWS = 32
VMEM_BUDGET = 48 * 1024 * 1024
VMEM_LIMIT = 60 * 1024 * 1024


def block_weights(image_rows, text_rows, positive, logit_scale, logit_bias):
    logits = (
        logit_scale * jnp.dot(image_rows, text_rows.T, preferred_element_type=jnp.float32)
        + logit_bias
    )
    signed = jnp.where(positive, jnp.float32(1.0), jnp.float32(-1.0))
    loss_sum = jnp.sum(jax.nn.softplus(-signed * logits))
    weight = (-signed * jax.nn.sigmoid(-signed * logits)).astype(jnp.bfloat16)
    return (loss_sum, weight)


def regroup(received, partner_row):
    row_count, width = received.shape
    devices = partner_row.shape[0]
    pieces = received.reshape(row_count, devices, width // devices)
    pieces = jnp.take(pieces, partner_row, axis=1)
    return pieces.reshape(row_count, width)


def spread_body(images, texts, labels, partners, logit_scale, logit_bias):
    own_images = images[0]
    own_texts = texts[0]
    row_count = own_images.shape[0]
    columns = jnp.arange(row_count, dtype=jnp.int32)
    positive = labels[0, 0][:, None] == columns[None, :]
    nothing = jnp.zeros((row_count, row_count), dtype=bool)
    loss_sum, weight = block_weights(own_images, own_texts, positive, logit_scale, logit_bias)
    image_grad = logit_scale * jnp.dot(weight, own_texts, preferred_element_type=jnp.float32)
    text_grad = logit_scale * jnp.dot(weight.T, own_images, preferred_element_type=jnp.float32)
    for round_index in range(partners.shape[0]):
        partner_row = partners[round_index]
        spread_images, spread_texts = (
            lax.all_to_all(own_images, "blk", split_axis=1, concat_axis=1, tiled=True),
            lax.all_to_all(own_texts, "blk", split_axis=1, concat_axis=1, tiled=True),
        )
        their_images, their_texts = (
            lax.all_to_all(
                regroup(spread_images, partner_row), "blk", split_axis=1, concat_axis=1, tiled=True
            ),
            lax.all_to_all(
                regroup(spread_texts, partner_row), "blk", split_axis=1, concat_axis=1, tiled=True
            ),
        )
        round_loss, weight = block_weights(
            own_images, their_texts, nothing, logit_scale, logit_bias
        )
        image_grad = image_grad + logit_scale * jnp.dot(
            weight, their_texts, preferred_element_type=jnp.float32
        )
        _, mirror = block_weights(
            their_images, own_texts, nothing, logit_scale, logit_bias
        )
        text_grad = text_grad + logit_scale * jnp.dot(
            mirror.T, their_images, preferred_element_type=jnp.float32
        )
        loss_sum = loss_sum + round_loss
    loss_all = lax.psum(loss_sum, ("blk", "grp"))
    image_count = lax.axis_size("blk") * lax.axis_size("grp") * row_count
    loss = loss_all / jnp.float32(image_count)
    return (image_grad[None], text_grad[None], loss)


def logistic_terms(value):
    small = jnp.exp(-jnp.abs(value))
    inverse = 1.0 / (1.0 + small)
    weight = jnp.where(value >= 0, inverse, small * inverse)
    return weight, jnp.maximum(value, 0.0) + jnp.log1p(small)


def rows_dot(rows, own):
    return lax.dot_general(rows, own, (((1,), (1,)), ((), ())), preferred_element_type=jnp.float32)


def weight_dot(weight, rows):
    return lax.dot_general(
        weight, rows, (((0,), (0,)), ((), ())), preferred_element_type=jnp.float32
    )


def fold(terms):
    rows, columns = terms.shape
    total = jnp.sum(terms.reshape(rows // 8, 8, columns), axis=0)
    return sum(total[:, c : c + 128] for c in range(0, columns, 128))


def exchange_kernel(
    n, groups, rounds, edges,
    partners_ref, scale_ref, bias_ref, labels_ref, images_ref, texts_ref,
    image_acc, text_acc, loss_ref,
    own, end_images, loss_sum, group_loss, block_loss,
    own_sem, load_sem, recv_sem, send_sem, slot_sem,
    group_send, group_recv, block_send, block_recv, *buffers,
):
    chunks = len(edges) - 1
    held, slots = buffers[:chunks], buffers[chunks:]
    chips = n // 2
    me = lax.axis_index("blk")
    grp = lax.axis_index("grp")
    chip = lax.div(me, 2)
    core = lax.rem(me, 2)
    sibling = me + 1 - 2 * core
    inner = jnp.logical_and(chip > 0, chip < chips - 1)
    outer = jnp.logical_not(inner)
    up_all = chip < chips - 2
    down_all = chip > 1
    beside_end = jnp.logical_or(chip == 1, chip == chips - 2)
    end_device = jnp.where(chip == 1, me - 2, me + 2)
    scale = scale_ref[0]
    bias = bias_ref[0]

    loads = []
    for k in range(chunks):
        part = pl.ds(edges[k], edges[k + 1] - edges[k])
        loads.append([
            pltpu.make_async_copy(ref.at[0, part], held[k].at[me, i], load_sem.at[k, i])
            for i, ref in enumerate((images_ref, texts_ref))
        ])
        for copy in loads[-1]:
            copy.start()
    own_loads = [
        pltpu.make_async_copy(ref.at[0], own.at[i], own_sem.at[i])
        for i, ref in enumerate((images_ref, texts_ref))
    ]
    for copy in own_loads:
        copy.start()

    barrier = pltpu.get_barrier_semaphore()
    for step in range(1, n):
        pl.semaphore_signal(
            barrier, inc=1, device_id={"blk": lax.rem(me + step, n)}, device_id_type=MESH
        )
    for step in range(1, groups):
        pl.semaphore_signal(
            barrier, inc=1, device_id={"grp": lax.rem(grp + step, groups)}, device_id_type=MESH
        )
    pl.semaphore_wait(barrier, n - 1 + groups - 1)

    pending = []

    def copy_of(k, entry, way, target):
        return pltpu.make_async_remote_copy(
            src_ref=held[k].at[entry],
            dst_ref=held[k].at[entry],
            send_sem=send_sem.at[k, way, lax.div(entry, 2)],
            recv_sem=recv_sem.at[k, entry],
            device_id={"blk": target},
            device_id_type=MESH,
        )

    def send(k, entry, way, target, when):
        pending.append((when, lambda: copy_of(k, entry, way, target).wait_send()))
        pl.when(when)(lambda: copy_of(k, entry, way, target).start())

    def arrived(k, entry, when):
        pl.when(when)(lambda: copy_of(k, entry, 0, sibling).wait_recv())

    def send_own(k, when):
        send(k, me, 0, me + 2, jnp.logical_and(when, up_all))
        send(k, me, 1, me - 2, jnp.logical_and(when, down_all))
        send(k, me, 2, sibling, jnp.logical_and(when, inner))

    def relay(k, passing):
        for distance in range(1, chips - 1):
            below = jnp.logical_and(inner, chip >= distance)
            below = jnp.logical_and(below, up_all == passing)
            arrived(k, me - 2 * distance, below)
            if passing:
                send(k, me - 2 * distance, 0, me + 2, below)
            send(k, me - 2 * distance, 2, sibling, below)
            above = jnp.logical_and(inner, chip + distance < chips)
            above = jnp.logical_and(above, down_all == passing)
            arrived(k, me + 2 * distance, above)
            if passing:
                send(k, me + 2 * distance, 1, me - 2, above)
            send(k, me + 2 * distance, 2, sibling, above)

    def slot_copy(k):
        return pltpu.make_async_remote_copy(
            src_ref=slots[k],
            dst_ref=held[k].at[pl.ds(n, rounds)],
            send_sem=slot_sem.at[k],
            recv_sem=recv_sem.at[k, n],
            device_id={"blk": end_device},
            device_id_type=MESH,
        )

    def select(k):
        for at in range(chips):
            arrived(k, 2 * at + 1 - core, inner)

        @pl.when(beside_end)
        def _():
            for r in range(rounds):
                slots[k][r] = held[k][partners_ref[r, end_device]]
            slot_copy(k).start()

        pl.when(outer)(lambda: slot_copy(k).wait_recv())

    def add_loss(terms):
        loss_sum[...] += fold(terms)

    def compute(k):
        found = [
            held[k][jnp.where(inner, partners_ref[r, me], n + r)] for r in range(rounds)
        ]
        their_images = jnp.concatenate([rows[0] for rows in found], axis=0)
        their_texts = jnp.concatenate([rows[1] for rows in found], axis=0)
        weight, terms = logistic_terms(scale * rows_dot(their_texts, own[0]) + bias)
        pl.when(inner)(lambda: add_loss(terms))
        mirror, _ = logistic_terms(scale * rows_dot(their_images, own[1]) + bias)
        image_acc[0] += weight_dot(weight.astype(jnp.bfloat16), their_texts)
        text_acc[0] += weight_dot(mirror.astype(jnp.bfloat16), their_images)

    always = me >= 0
    for k in range(chunks):
        for copy in loads[k]:
            copy.wait()
        send_own(k, always if k < 2 else outer)

    def own_pair():
        logits = scale * rows_dot(own[1], own[0]) + bias
        positive = lax.broadcasted_iota(jnp.int32, logits.shape, 0) == labels_ref[0]
        signed = jnp.where(positive, -1.0, 1.0)
        weight, terms = logistic_terms(signed * logits)
        weight = (signed * weight).astype(jnp.bfloat16)
        loss_sum[...] = fold(terms)
        image_acc[0] = weight_dot(weight, own[1])
        text_acc[0] = jnp.dot(weight, own[0], preferred_element_type=jnp.float32)

    def end_rows():
        for k in range(chunks):
            end_images[edges[k] : edges[k + 1]] = held[k][end_device, 0]

    def end_loss(k):
        texts = jnp.concatenate([slots[k][r, 1] for r in range(rounds)], axis=0)
        _, terms = logistic_terms(scale * rows_dot(texts, end_images[...]) + bias)
        loss_sum[...] += fold(terms)

    def share(slot, position, count, axis, send, recv):
        def copy(step, index):
            return pltpu.make_async_remote_copy(
                src_ref=slot.at[index],
                dst_ref=slot.at[index],
                send_sem=send.at[step],
                recv_sem=recv.at[index],
                device_id={axis: lax.rem(position + step, count)},
                device_id_type=MESH,
            )

        def start():
            for step in range(1, count):
                copy(step, position).start()

        def finish():
            for step in range(1, count):
                copy(step, lax.rem(position + step, count)).wait_recv()
            for step in range(1, count):
                copy(step, position).wait_send()
            total = slot[0]
            for at in range(1, count):
                total = total + slot[at]
            return total

        return start, finish

    group_start, group_finish = share(group_loss, grp, groups, "grp", group_send, group_recv)
    block_start, block_finish = share(block_loss, me, n, "blk", block_send, block_recv)

    def send_loss():
        group_loss[grp] = loss_sum[...]
        group_start()
        block_loss[me] = group_finish()
        block_start()

    for copy in own_loads:
        copy.wait()
    half = chunks // 2
    ahead = 0
    for k in range(chunks):
        while ahead < min(2 * k + 2, chunks):
            relay(ahead, True)
            if 0 < ahead < chunks - 1:
                send_own(ahead + 1, inner)
            ahead += 1
        if k == 0:
            pl.when(outer)(own_pair)
            pl.when(outer)(send_loss)
        relay(k, False)
        select(k)
        if k == 0:
            pl.when(inner)(own_pair)
        compute(k)
        if k == half:
            pl.when(beside_end)(end_rows)
        if k >= half:
            for j in (2 * (k - half), 2 * (k - half) + 1):
                if j < chunks:
                    pl.when(beside_end)(functools.partial(end_loss, j))
    pl.when(inner)(send_loss)
    loss_ref[0, 0] = jnp.sum(block_finish()) / jnp.float32(n * groups * own.shape[1])

    for when, wait in pending:
        pl.when(when)(wait)
    for k in range(chunks):
        pl.when(beside_end)(lambda k=k: slot_copy(k).wait_send())


def chunk_edges(rows):
    half = CHUNK_ROWS // 2
    return [0] + list(range(half, rows, CHUNK_ROWS)) + [rows]


def gather_body(n, groups, images, texts, labels, partners, logit_scale, logit_bias):
    _, rows, width = images.shape
    rounds = partners.shape[0]
    edges = chunk_edges(rows)
    chunks = len(edges) - 1
    sizes = [edges[k + 1] - edges[k] for k in range(chunks)]
    vmem = pl.BlockSpec(memory_space=pltpu.VMEM)
    smem = pl.BlockSpec(memory_space=pltpu.SMEM)
    hbm = pl.BlockSpec(memory_space=pl.ANY)
    dma = pltpu.SemaphoreType.DMA
    grad = jax.ShapeDtypeStruct(images.shape, jnp.float32)
    image_grad, text_grad, loss = pl.pallas_call(
        functools.partial(exchange_kernel, n, groups, rounds, edges),
        out_shape=(grad, grad, jax.ShapeDtypeStruct((1, 1), jnp.float32)),
        in_specs=[smem, smem, smem, vmem, hbm, hbm],
        out_specs=(vmem, vmem, smem),
        scratch_shapes=[
            pltpu.VMEM((2, rows, width), images.dtype),
            pltpu.VMEM((rows, width), images.dtype),
            pltpu.VMEM((8, 128), jnp.float32),
            pltpu.VMEM((groups, 8, 128), jnp.float32),
            pltpu.VMEM((n, 8, 128), jnp.float32),
            dma((2,)),
            dma((chunks, 2)),
            dma((chunks, n + 1)),
            dma((chunks, 3, n // 2)),
            dma((chunks,)),
            dma((groups,)),
            dma((groups,)),
            dma((n,)),
            dma((n,)),
        ]
        + [pltpu.VMEM((n + rounds, 2, size, width), images.dtype) for size in sizes]
        + [pltpu.VMEM((rounds, 2, size, width), images.dtype) for size in sizes],
        compiler_params=pltpu.CompilerParams(
            collective_id=0, has_side_effects=True, vmem_limit_bytes=VMEM_LIMIT
        ),
    )(partners, logit_scale.reshape(1), logit_bias.reshape(1), labels, images, texts)
    return logit_scale * image_grad, logit_scale * text_grad, loss.reshape(())


def solution(mesh):
    in_specs = (P("grp", "blk", None), P("grp", "blk", None), P("grp", "blk", None), P(), P(), P())
    out_specs = (P("grp", "blk", None), P("grp", "blk", None), P())
    n, groups = mesh.shape["blk"], mesh.shape["grp"]

    def body(images, texts, labels, partners, logit_scale, logit_bias):
        _, rows, width = images.shape
        rounds = partners.shape[0]
        block = 2 * rows * width * images.dtype.itemsize
        needed = block * (n + 2 * rounds + 1) + 2 * rows * width * 4
        fits = needed <= VMEM_BUDGET and n % 2 == 0 and n >= 8
        if fits and rows % CHUNK_ROWS == 0 and rows % 128 == 0 and width % 128 == 0:
            return gather_body(
                n, groups, images, texts, labels, partners, logit_scale, logit_bias
            )
        return spread_body(images, texts, labels, partners, logit_scale, logit_bias)

    return jax.shard_map(body, mesh=mesh, in_specs=in_specs, out_specs=out_specs, check_vma=False)
```
